32 devices in a mesh: gz: 32 (over z, y, x, core).
Axes of the slice: x: 2, y: 2, z: 4, core: 2. Of those that a mesh axis runs over, the one named last changes fastest.
Arguments:
- coefficient: float32 [64, 512, 512], P('gz'), may hold values from 0.2 to 1.3
- initial_field: float32 [64, 512, 512], P('gz'), may hold values from -6 to 6
- observed: float32 [64, 512, 512], P('gz'), may hold values from -6 to 6
- misfit_weight: float32 [64, 512, 512], P('gz'), may hold values from 0.5 to 6, as said below
Outputs:
- coeff_gradient: float32 [64, 512, 512], P('gz')
- adjoint_field: float32 [64, 512, 512], P('gz')
- misfit: float32 [], replicated
The draws below stay inside these ranges and needn't reach their ends.
Inputs may be any that keep to these rules, and one draw needn't show every extreme that they name: `misfit_weight`: positive cell weights.
All inputs are finite; a program needn't handle non-finite values.
Results may differ from the reference program's by a relative error of at most 0.00002.
Values sent between devices are 32-bit elements; how exact they have to be, the bound alone decides.
A program may use at most 128 MiB of HBM per device.

```python
import math
import jax
import jax.numpy as jnp

NY = 512
NX = 512
ITERS = 4
NZ = 64


def draw_misfit_weight(key, part):
    depth = jnp.arange(NZ, dtype=jnp.float32)[:, None, None]
    ramp = 1.0 + 2.0 * depth / (NZ - 1)
    base = jnp.exp(jax.random.uniform(key, (NZ, NY, NX), jnp.float32, jnp.log(0.5), jnp.log(2.0)))
    return (ramp * base).astype(jnp.float32)


def block_scale(stream_key, shape, split, smallest, high):
    def one(axis_at, parts):
        steps = jax.random.uniform(jax.random.fold_in(jax.random.fold_in(stream_key, 6), axis_at), (parts,), jnp.float32, smallest / len(split), high / len(split))
        return jnp.repeat(jnp.exp(steps), shape[axis_at] // parts).reshape((-1,) + (1,) * (len(shape) - axis_at - 1))

    gain = one(*split[0])
    for cut in split[1:]:
        gain = gain * one(*cut)
    return gain


def centred(key, extent, width, bound, split=(), kind=jnp.bfloat16):
    array = width * jax.random.normal(key, extent, jnp.float32)
    if split:
        array = array * block_scale(key, extent, split, -0.22, 0.18)
    return jnp.clip(array, -bound, bound).astype(kind)


def setup_inputs(seed: int = 0) -> dict:
    splits = jax.random.split(jax.random.key(seed), 5)
    coefficient = jnp.clip(jnp.exp(math.log(1.3) - 1.8718021 * jax.random.uniform(splits[0], (NZ, NY, NX), jnp.float32) ** block_scale(splits[0], (NZ, NY, NX), ((0, 32),), -0.2, 0.2)), 0.2, 1.3)
    initial_field = centred(splits[1], (NZ, NY, NX), 1.0, 6.0, ((0, 32),), jnp.float32)
    observed = centred(splits[2], (NZ, NY, NX), 1.0, 6.0, ((0, 32),), jnp.float32)
    misfit_weight = draw_misfit_weight(jax.random.fold_in(splits[4], 71), 0)
    return {"coefficient": coefficient, "initial_field": initial_field, "observed": observed, "misfit_weight": misfit_weight}


time_step = 0.125

def laplace(field):
    padded = jnp.pad(field, 1)
    beside = padded[2:, 1:-1, 1:-1] + padded[:-2, 1:-1, 1:-1]
    beside = beside + padded[1:-1, 2:, 1:-1] + padded[1:-1, :-2, 1:-1]
    beside = beside + padded[1:-1, 1:-1, 2:] + padded[1:-1, 1:-1, :-2]
    return beside - 6.0 * field

def reference(coefficient, initial_field, observed, misfit_weight):
    state = initial_field
    slopes = []
    for step in range(ITERS):
        slope = laplace(state)
        slopes.append(slope)
        state = state + time_step * coefficient * slope
    resid = state - observed
    total = jnp.sum(misfit_weight * resid * resid)
    misfit = jnp.sqrt(total / (NZ * NY * NX) + 1e-06)
    adjoint = misfit_weight * resid / misfit
    gradient = jnp.zeros_like(coefficient)
    for step in reversed(range(ITERS)):
        gradient = gradient + time_step * adjoint * slopes[step]
        adjoint = adjoint + time_step * laplace(coefficient * adjoint)
    return (gradient, adjoint, misfit)
```

```python
import functools

import jax
import jax.numpy as jnp
from jax import lax
from jax.experimental import pallas as pl
from jax.experimental.pallas import tpu as pltpu
from jax.sharding import PartitionSpec as P

ITERS = 4
time_step = 0.125
MESH = pl.DeviceIdType.MESH
PAD = 8
CHUNKS = 8
TILE = 16


def kernel(n, rounds, cells, coef_hbm, init_hbm, obs_hbm, wgt_hbm, grad, adj, misfit_out,
           st, sl, halo, coef, obs, wgt, part, send_sem, recv_sem, psend_sem, precv_sem, load_sem):
    planes, ny, nx = coef_hbm.shape
    rows = ny // CHUNKS
    exchanges = 2 * ITERS
    me = lax.axis_index("gz")
    has_lo = me > 0
    has_hi = me < n - 1

    loads = [
        pltpu.make_async_copy(init_hbm, st.at[0, :, pl.ds(PAD, ny), :], load_sem.at[0]),
        pltpu.make_async_copy(coef_hbm, coef, load_sem.at[1]),
        pltpu.make_async_copy(obs_hbm, obs, load_sem.at[2]),
        pltpu.make_async_copy(wgt_hbm, wgt, load_sem.at[3]),
    ]

    partners = []
    for r in range(rounds):
        bit = 1 << r
        partners.append(me + bit * (1 - 2 * ((me // bit) % 2)))

    barrier = pltpu.get_barrier_semaphore()

    def greet(device):
        pl.semaphore_signal(barrier, inc=1, device_id=(device,), device_id_type=MESH)

    @pl.when(has_lo)
    def _():
        greet(me - 1)

    @pl.when(has_hi)
    def _():
        greet(me + 1)

    for partner in partners[1:]:
        greet(partner)
    for load in loads:
        load.start()

    zero_rows = jnp.zeros((PAD, nx), jnp.float32)

    def clear_pad(e, carry):
        for p in range(planes):
            st[e, p, pl.ds(0, PAD), :] = zero_rows
            st[e, p, pl.ds(PAD + ny, PAD), :] = zero_rows
        return carry

    lax.fori_loop(0, exchanges, clear_pad, 0)

    def clear_halo(side):
        def clear(i, carry):
            e = i // (ny // PAD)
            row = pl.multiple_of((i % (ny // PAD)) * PAD, PAD)
            halo[side, e, pl.ds(row, PAD), :] = zero_rows
            return carry

        lax.fori_loop(0, exchanges * (ny // PAD), clear, 0)

    @pl.when(me == 0)
    def _():
        clear_halo(0)

    @pl.when(me == n - 1)
    def _():
        clear_halo(1)

    @pl.when(has_lo & has_hi)
    def _():
        pl.semaphore_wait(barrier, rounds + 1)

    if rounds:
        @pl.when((me == 0) | (me == n - 1))
        def _():
            pl.semaphore_wait(barrier, rounds)

    def remote(side, e, j, src):
        at = pl.ds(pl.multiple_of(j * rows, rows), rows)
        return pltpu.make_async_remote_copy(
            src_ref=src,
            dst_ref=halo.at[side, e, at, :],
            send_sem=send_sem.at[side, e, j],
            recv_sem=recv_sem.at[side, e, j],
            device_id=(me + 1 - 2 * side,),
            device_id_type=MESH,
        )

    def source(side, e, j):
        at = pl.ds(pl.multiple_of(PAD + j * rows, PAD), rows)
        return st.at[e, (planes - 1) * (1 - side), at, :]

    def first_source(side, j):
        return init_hbm.at[(planes - 1) * (1 - side), pl.ds(pl.multiple_of(j * rows, rows), rows), :]

    def send_first(j, carry):
        @pl.when(has_hi)
        def _():
            remote(0, 0, j, first_source(0, j)).start()

        @pl.when(has_lo)
        def _():
            remote(1, 0, j, first_source(1, j)).start()

        return carry

    lax.fori_loop(0, CHUNKS, send_first, 0)

    def send(e, j):
        @pl.when(has_hi)
        def _():
            remote(0, e, j, source(0, e, j)).start()

        @pl.when(has_lo)
        def _():
            remote(1, e, j, source(1, e, j)).start()

    def receive(e, j):
        @pl.when(has_lo)
        def _():
            remote(0, e, j, source(0, e, j)).wait_recv()

        @pl.when(has_hi)
        def _():
            remote(1, e, j, source(1, e, j)).wait_recv()

    lane = lax.broadcasted_iota(jnp.int32, (TILE, nx), 1)
    leftmost = lane == 0
    rightmost = lane == nx - 1

    def tile_laplace(e, row):
        here = pl.ds(row, TILE)
        tall = [st[e, p, pl.ds(row, TILE + 2 * PAD), :] for p in range(planes)]
        mids = [t[PAD:PAD + TILE] for t in tall]
        result = []
        for p in range(planes):
            mid = mids[p]
            beside = tall[p][PAD + 1:PAD + 1 + TILE] + tall[p][PAD - 1:PAD - 1 + TILE]
            beside = beside + jnp.where(rightmost, 0.0, pltpu.roll(mid, nx - 1, 1))
            beside = beside + jnp.where(leftmost, 0.0, pltpu.roll(mid, 1, 1))
            above = mids[p + 1] if p + 1 < planes else halo[1, e, here, :]
            below = mids[p - 1] if p > 0 else halo[0, e, here, :]
            result.append((mid, beside + above + below - 6.0 * mid))
        return result

    def over_tiles(j, body, carry):
        def one(t, carry):
            row = pl.multiple_of(j * rows + t * TILE, TILE)
            return body(row, carry)

        return lax.fori_loop(0, rows // TILE, one, carry)

    loads[0].wait()
    loads[1].wait()

    def forward(e, carry):
        def chunk(j, carry):
            receive(e, j)

            def body(row, carry):
                here, padded = pl.ds(row, TILE), pl.ds(pl.multiple_of(row + PAD, PAD), TILE)
                for p, (mid, slope) in enumerate(tile_laplace(e, row)):
                    sl[e, p, here, :] = slope
                    st[e + 1, p, padded, :] = mid + time_step * coef[p, here, :] * slope
                return carry

            over_tiles(j, body, 0)
            send(e + 1, j)
            return carry

        return lax.fori_loop(0, CHUNKS, chunk, carry)

    lax.fori_loop(0, ITERS - 1, forward, 0)
    loads[2].wait()
    loads[3].wait()

    last = ITERS - 1

    def turn(j, total):
        receive(last, j)

        def body(row, total):
            here, padded = pl.ds(row, TILE), pl.ds(pl.multiple_of(row + PAD, PAD), TILE)
            for p, (mid, slope) in enumerate(tile_laplace(last, row)):
                c = coef[p, here, :]
                resid = mid + time_step * c * slope - obs[p, here, :]
                weighted = wgt[p, here, :] * resid
                total = total + weighted * resid
                adj[p, here, :] = weighted
                grad[p, here, :] = time_step * weighted * slope
                st[ITERS, p, padded, :] = c * weighted
            return total

        total = over_tiles(j, body, total)
        send(ITERS, j)
        return total

    total = lax.fori_loop(0, CHUNKS, turn, jnp.zeros((TILE, nx), jnp.float32))
    folded = total[0:8]
    for i in range(1, TILE // 8):
        folded = folded + total[8 * i:8 * i + 8]
    narrow = folded[:, 0:128]
    for i in range(1, nx // 128):
        narrow = narrow + folded[:, 128 * i:128 * i + 128]
    part[0] = narrow

    def exchange(r):
        return pltpu.make_async_remote_copy(
            src_ref=part.at[2 * r],
            dst_ref=part.at[2 * r + 1],
            send_sem=psend_sem.at[r],
            recv_sem=precv_sem.at[r],
            device_id=(partners[r],),
            device_id_type=MESH,
        )

    def adjoint_chunk(e, j):
        receive(e, j)

        def body(row, carry):
            here, padded = pl.ds(row, TILE), pl.ds(pl.multiple_of(row + PAD, PAD), TILE)
            for p, (_, change) in enumerate(tile_laplace(e, row)):
                lam = adj[p, here, :] + time_step * change
                adj[p, here, :] = lam
                grad[p, here, :] = grad[p, here, :] + time_step * lam * sl[exchanges - 2 - e, p, here, :]
                st[e + 1, p, padded, :] = coef[p, here, :] * lam
            return carry

        over_tiles(j, body, 0)
        send(e + 1, j)

    done = 0
    for j in range(CHUNKS):
        adjoint_chunk(ITERS, j)
        if j < rounds:
            if j > 0:
                exchange(j - 1).wait_recv()
                part[2 * j] = part[2 * j - 2] + part[2 * j - 1]
            exchange(j).start()
            done = j + 1
    for r in range(done, rounds):
        exchange(r - 1).wait_recv()
        part[2 * r] = part[2 * r - 2] + part[2 * r - 1]
        exchange(r).start()

    def backward(e, carry):
        def chunk(j, carry):
            adjoint_chunk(e, j)
            return carry

        return lax.fori_loop(0, CHUNKS, chunk, carry)

    lax.fori_loop(ITERS + 1, exchanges - 1, backward, 0)

    if rounds:
        exchange(rounds - 1).wait_recv()
        whole = part[2 * rounds - 2] + part[2 * rounds - 1]
    else:
        whole = part[0]
    whole = jnp.sum(jnp.sum(whole, axis=1, keepdims=True), axis=0, keepdims=True)
    misfit = jnp.sqrt(jnp.broadcast_to(whole, (8, 128)) / cells + 1e-06)
    misfit_out[...] = misfit

    def final(j, carry):
        receive(exchanges - 1, j)

        def body(row, carry):
            here = pl.ds(row, TILE)
            for p, (_, change) in enumerate(tile_laplace(exchanges - 1, row)):
                adj[p, here, :] = adj[p, here, :] + time_step * change
            return carry

        return over_tiles(j, body, carry)

    lax.fori_loop(0, CHUNKS, final, 0)

    def drain(j, carry):
        for e in range(exchanges):
            @pl.when(has_hi)
            def _():
                remote(0, e, j, first_source(0, j) if e == 0 else source(0, e, j)).wait_send()

            @pl.when(has_lo)
            def _():
                remote(1, e, j, first_source(1, j) if e == 0 else source(1, e, j)).wait_send()

        return carry

    lax.fori_loop(0, CHUNKS, drain, 0)
    for r in range(rounds):
        exchange(r).wait_send()


def solution(mesh):
    n = mesh.shape["gz"]
    rounds = n.bit_length() - 1

    def on_device(coefficient, initial_field, observed, misfit_weight):
        planes, ny, nx = coefficient.shape
        slab = jax.ShapeDtypeStruct(coefficient.shape, jnp.float32)
        exchanges = 2 * ITERS
        grad, adj, misfit = pl.pallas_call(
            functools.partial(kernel, n, rounds, float(n * planes * ny * nx)),
            out_shape=(slab, slab, jax.ShapeDtypeStruct((8, 128), jnp.float32)),
            in_specs=[pl.BlockSpec(memory_space=pl.ANY)] * 4,
            out_specs=[pl.BlockSpec(memory_space=pltpu.VMEM)] * 3,
            scratch_shapes=[
                pltpu.VMEM((exchanges, planes, ny + 2 * PAD, nx), jnp.float32),
                pltpu.VMEM((ITERS - 1, planes, ny, nx), jnp.float32),
                pltpu.VMEM((2, exchanges, ny, nx), jnp.float32),
                pltpu.VMEM((planes, ny, nx), jnp.float32),
                pltpu.VMEM((planes, ny, nx), jnp.float32),
                pltpu.VMEM((planes, ny, nx), jnp.float32),
                pltpu.VMEM((2 * max(rounds, 1), 8, 128), jnp.float32),
                pltpu.SemaphoreType.DMA((2, exchanges, CHUNKS)),
                pltpu.SemaphoreType.DMA((2, exchanges, CHUNKS)),
                pltpu.SemaphoreType.DMA((max(rounds, 1),)),
                pltpu.SemaphoreType.DMA((max(rounds, 1),)),
                pltpu.SemaphoreType.DMA((4,)),
            ],
            compiler_params=pltpu.CompilerParams(
                collective_id=0, has_side_effects=True, vmem_limit_bytes=67043328
            ),
        )(coefficient, initial_field, observed, misfit_weight)
        scale = misfit[0, 0]
        return grad / scale, adj / scale, scale

    placed = P("gz", None, None)
    return jax.shard_map(
        on_device,
        mesh=mesh,
        in_specs=(placed,) * 4,
        out_specs=(placed, placed, P()),
        check_vma=False,
    )
```

```python
import functools

import jax
import jax.numpy as jnp
from jax import lax
from jax.experimental import pallas as pl
from jax.experimental.pallas import tpu as pltpu
from jax.sharding import PartitionSpec as P

ITERS = 4
time_step = 0.125
MESH = pl.DeviceIdType.MESH
PAD = 8
TILE = 8
CHUNKS = 16


def kernel(n, rounds, cells, coef_hbm, init_hbm, obs_hbm, wgt_hbm, grad_out, adj_out, misfit_out,
           st, sl, halo, coef, obs, wgt, gacc, aacc, acc, part, edge_out, edge_in,
           in_send, in_recv, halo_send, halo_recv, edge_send, edge_recv,
           out_send, out_recv, psend_sem, precv_sem):
    own, ny, nx = coef_hbm.shape
    planes, half = 2 * own, ny // 2
    rows = half // CHUNKS
    exchanges = 2 * ITERS
    me = lax.axis_index("gz")
    q = me % 4
    base = me - q
    h, s = q // 2, q % 2
    lower, upper = me - 3 + 2 * s, me + 1 + 2 * s
    mate = me + 2 - 4 * h
    has_lo = lower >= 0
    has_hi = upper < n
    partners = []
    for r in range(rounds):
        bit = 1 << r
        partners.append(me + bit * (1 - 2 * ((me // bit) % 2)))

    barrier = pltpu.get_barrier_semaphore()

    def greet(device):
        pl.semaphore_signal(barrier, inc=1, device_id=(device,), device_id_type=MESH)

    for i in range(1, 4):
        greet(base + (q + i) % 4)
    for partner in partners[2:]:
        greet(partner)
    outside_lo = (s == 0) & has_lo
    outside_hi = (s == 1) & has_hi

    @pl.when(outside_lo)
    def _():
        greet(lower)

    @pl.when(outside_hi)
    def _():
        greet(upper)

    zero_rows = jnp.zeros((PAD, nx), jnp.float32)
    outer = pl.multiple_of(h * (PAD + half), PAD)
    inner = pl.multiple_of((1 - h) * (PAD + half), PAD)

    def clear_pad(e, carry):
        for p in range(planes):
            st[e, p, pl.ds(outer, PAD), :] = zero_rows
        return carry

    lax.fori_loop(0, exchanges, clear_pad, 0)

    def clear_halo(side):
        def clear(i, carry):
            e = i // (half // PAD)
            row = pl.multiple_of((i % (half // PAD)) * PAD, PAD)
            halo[side, e, pl.ds(row, PAD), :] = zero_rows
            return carry

        lax.fori_loop(0, exchanges * (half // PAD), clear, 0)

    @pl.when(jnp.logical_not(has_lo))
    def _():
        clear_halo(0)

    @pl.when(jnp.logical_not(has_hi))
    def _():
        clear_halo(1)

    acc[...] = jnp.zeros_like(acc)
    crossing = outside_lo | outside_hi

    @pl.when(crossing)
    def _():
        pl.semaphore_wait(barrier, rounds + 2)

    @pl.when(jnp.logical_not(crossing))
    def _():
        pl.semaphore_wait(barrier, rounds + 1)

    hbm = (init_hbm, coef_hbm, obs_hbm, wgt_hbm)
    held = (None, coef, obs, wgt)

    def place(side_half, j):
        return j if side_half == 1 else CHUNKS - 1 - j

    def feed(array, j):
        for to in range(2):
            dest = base + 2 * to + q // 2
            row = place(to, j) * rows
            slot = pl.ds(s * own, own)
            if array == 0:
                if isinstance(j, int) and j == 0:
                    start = row if to == 0 else half - PAD
                    src = init_hbm.at[:, pl.ds(start, rows + PAD), :]
                    dst = st.at[0, slot, pl.ds(PAD + row if to == 0 else 0, rows + PAD), :]
                else:
                    src = init_hbm.at[:, pl.ds(pl.multiple_of(to * half + row, PAD), rows), :]
                    dst = st.at[0, slot, pl.ds(pl.multiple_of(PAD + row, PAD), rows), :]
            else:
                src = hbm[array].at[:, pl.ds(pl.multiple_of(to * half + row, PAD), rows), :]
                dst = held[array].at[slot, pl.ds(pl.multiple_of(row, PAD), rows), :]
            arrived = in_recv.at[array, s, j]

            @pl.when(dest == me)
            def _():
                pltpu.make_async_copy(src, dst, arrived).start()

            @pl.when(dest != me)
            def _():
                pltpu.make_async_remote_copy(
                    src_ref=src, dst_ref=dst, send_sem=in_send.at[array, to], recv_sem=arrived,
                    device_id=(dest,), device_id_type=MESH,
                ).start()

    def await_copy(ref, sem):
        pltpu.make_async_copy(ref, ref, sem).wait()

    def fed(array, j, at):
        for slot in range(2):
            arrived = in_recv.at[array, slot, j]
            mine = pl.ds(slot * own, own)
            if array == 0:
                @pl.when(j == 0)
                def _():
                    start = pl.multiple_of((1 - h) * (PAD + at), PAD)
                    await_copy(st.at[0, mine, pl.ds(start, rows + PAD), :], arrived)

                @pl.when(j != 0)
                def _():
                    await_copy(st.at[0, mine, pl.ds(pl.multiple_of(PAD + at, PAD), rows), :], arrived)
            else:
                await_copy(held[array].at[mine, pl.ds(at, rows), :], arrived)

    for j in range(2):
        feed(0, j)
        feed(1, j)

    def send(e, at, j):
        here = pl.ds(at, rows)
        padded = pl.ds(pl.multiple_of(PAD + at, PAD), rows)

        def copy(side, device):
            pltpu.make_async_remote_copy(
                src_ref=st.at[e, (planes - 1) * (1 - side), padded, :],
                dst_ref=halo.at[side, e, here, :],
                send_sem=halo_send.at[side, e], recv_sem=halo_recv.at[side, e, j],
                device_id=(device,), device_id_type=MESH,
            ).start()

        @pl.when(has_hi)
        def _():
            copy(0, upper)

        @pl.when(has_lo)
        def _():
            copy(1, lower)

    def receive(e, at, j):
        here = pl.ds(at, rows)

        @pl.when(has_lo)
        def _():
            await_copy(halo.at[0, e, here, :], halo_recv.at[0, e, j])

        @pl.when(has_hi)
        def _():
            await_copy(halo.at[1, e, here, :], halo_recv.at[1, e, j])

    def edge_copy(e):
        return pltpu.make_async_remote_copy(
            src_ref=edge_out.at[e], dst_ref=edge_in.at[e],
            send_sem=edge_send.at[e], recv_sem=edge_recv.at[e],
            device_id=(mate,), device_id_type=MESH,
        )

    def stage_edge(e):
        at = pl.multiple_of(PAD + (1 - h) * (half - PAD), PAD)
        for p in range(planes):
            block = st[e, p, pl.ds(at, PAD), :]
            edge_out[e, p:p + 1, :] = jnp.where(h == 0, block[PAD - 1:PAD], block[0:1])

    def take_edge(e):
        edge_copy(e).wait_recv()
        for p in range(planes):
            st[e, p, pl.ds(inner, PAD), :] = jnp.broadcast_to(edge_in[e, p:p + 1, :], (PAD, nx))

    lane = lax.broadcasted_iota(jnp.int32, (TILE, nx), 1)
    leftmost = lane == 0
    rightmost = lane == nx - 1

    def laplace(e, p, row):
        here = pl.ds(row, TILE)
        padded = pl.ds(pl.multiple_of(row + PAD, PAD), TILE)
        tall = st[e, p, pl.ds(row, TILE + 2 * PAD), :]
        mid = tall[PAD:PAD + TILE]
        beside = tall[PAD + 1:PAD + 1 + TILE] + tall[PAD - 1:PAD - 1 + TILE]
        beside = beside + jnp.where(rightmost, 0.0, pltpu.roll(mid, nx - 1, 1))
        beside = beside + jnp.where(leftmost, 0.0, pltpu.roll(mid, 1, 1))
        above = st[e, p + 1, padded, :] if p + 1 < planes else halo[1, e, here, :]
        below = st[e, p - 1, padded, :] if p > 0 else halo[0, e, here, :]
        return mid, beside + above + below - 6.0 * mid

    def ship(which, source, target, at):
        for o in range(2):
            dest = base + 2 * s + o
            src = source.at[pl.ds(o * own, own), pl.ds(at, rows), :]
            dst = target.at[:, pl.ds(pl.multiple_of(h * half + at, PAD), rows), :]

            @pl.when(dest == me)
            def _():
                pltpu.make_async_copy(src, dst, out_recv.at[which, h]).start()

            @pl.when(dest != me)
            def _():
                pltpu.make_async_remote_copy(
                    src_ref=src, dst_ref=dst, send_sem=out_send.at[which, o],
                    recv_sem=out_recv.at[which, h], device_id=(dest,), device_id_type=MESH,
                ).start()

    def stage(e, j):
        at = pl.multiple_of((CHUNKS - 1 - j) * (1 - h) * rows + j * h * rows, PAD)
        if e == 0:
            fed(1, j, at)
        else:
            @pl.when(j == 0)
            def _():
                take_edge(e)
        if e == ITERS - 1:
            fed(2, j, at)
            fed(3, j, at)
        receive(e, at, j)

        def tile(t, carry):
            row = pl.multiple_of(at + t * TILE, TILE)
            here = pl.ds(row, TILE)
            padded = pl.ds(pl.multiple_of(row + PAD, PAD), TILE)
            for p in range(planes):
                mid, slope = laplace(e, p, row)
                if e < ITERS - 1:
                    sl[e, p, here, :] = slope
                    st[e + 1, p, padded, :] = mid + time_step * coef[p, here, :] * slope
                elif e == ITERS - 1:
                    c = coef[p, here, :]
                    resid = mid + time_step * c * slope - obs[p, here, :]
                    weighted = wgt[p, here, :] * resid
                    acc[...] += weighted * resid
                    aacc[p, here, :] = weighted
                    gacc[p, here, :] = time_step * weighted * slope
                    st[e + 1, p, padded, :] = c * weighted
                else:
                    lam = aacc[p, here, :] + time_step * slope
                    aacc[p, here, :] = lam
                    if e < exchanges - 1:
                        gacc[p, here, :] += time_step * lam * sl[exchanges - 2 - e, p, here, :]
                        st[e + 1, p, padded, :] = coef[p, here, :] * lam
            return carry

        lax.fori_loop(0, rows // TILE, tile, 0)
        if e < exchanges - 1:
            @pl.when(j == 0)
            def _():
                stage_edge(e + 1)

            send(e + 1, at, j)

            @pl.when(j == 0)
            def _():
                edge_copy(e + 1).start()
        if e == exchanges - 2:
            ship(0, gacc, grad_out, at)
        if e == exchanges - 1:
            ship(1, aacc, adj_out, at)

    def exchange(r):
        return pltpu.make_async_remote_copy(
            src_ref=part.at[2 * r], dst_ref=part.at[2 * r + 1],
            send_sem=psend_sem.at[r], recv_sem=precv_sem.at[r],
            device_id=(partners[r],), device_id_type=MESH,
        )

    def total_round(r):
        if r == 0:
            whole = acc[...]
            narrow = whole[:, 0:128]
            for i in range(1, nx // 128):
                narrow = narrow + whole[:, 128 * i:128 * i + 128]
            part[0] = narrow
        else:
            exchange(r - 1).wait_recv()
            part[2 * r] = part[2 * r - 2] + part[2 * r - 1]
        exchange(r).start()

    summed = CHUNKS + ITERS - 1
    ticks = CHUNKS + exchanges

    def tick(t, carry):
        @pl.when(t < CHUNKS)
        def _():
            at = pl.multiple_of((CHUNKS - 1 - t) * (1 - h) * rows + t * h * rows, PAD)
            fed(0, t, at)
            send(0, at, t)

        for e in range(exchanges):
            j = t - 1 - e

            @pl.when((j >= 0) & (j < CHUNKS))
            def _():
                stage(e, j)

        @pl.when(t + 2 < CHUNKS)
        def _():
            feed(0, t + 2)
            feed(1, t + 2)

        late = t + 1 - ITERS + 1

        @pl.when((late >= 0) & (late < CHUNKS))
        def _():
            feed(2, late)
            feed(3, late)

        for r in range(min(rounds, ticks - summed)):
            @pl.when(t == summed + r)
            def _():
                total_round(r)

        return carry

    lax.fori_loop(0, ticks, tick, 0)
    for r in range(ticks - summed, rounds):
        total_round(r)

    exchange(rounds - 1).wait_recv()
    whole = part[2 * rounds - 2] + part[2 * rounds - 1]
    whole = jnp.sum(jnp.sum(whole, axis=1, keepdims=True), axis=0, keepdims=True)
    misfit_out[...] = jnp.sqrt(jnp.broadcast_to(whole, (8, 128)) / cells + 1e-06)

    for which, target in enumerate((grad_out, adj_out)):
        for side in range(2):
            await_copy(target.at[:, pl.ds(side * half, half), :], out_recv.at[which, side])
    for which, source in enumerate((gacc, aacc)):
        for o in range(2):
            @pl.when(base + 2 * s + o != me)
            def _():
                await_copy(source.at[pl.ds(o * own, own)], out_send.at[which, o])
    for array in range(4):
        for to in range(2):
            @pl.when(base + 2 * to + q // 2 != me)
            def _():
                extra = PAD if array == 0 else 0
                await_copy(hbm[array].at[:, pl.ds(0, half + extra), :], in_send.at[array, to])
    for e in range(exchanges):
        @pl.when(has_hi)
        def _():
            await_copy(halo.at[0, e], halo_send.at[0, e])

        @pl.when(has_lo)
        def _():
            await_copy(halo.at[1, e], halo_send.at[1, e])
    for e in range(1, exchanges):
        edge_copy(e).wait_send()
    for r in range(rounds):
        exchange(r).wait_send()


def solution(mesh):
    n = mesh.shape["gz"]
    rounds = n.bit_length() - 1

    def on_device(coefficient, initial_field, observed, misfit_weight):
        own, ny, nx = coefficient.shape
        planes, half = 2 * own, ny // 2
        slab = jax.ShapeDtypeStruct(coefficient.shape, jnp.float32)
        exchanges = 2 * ITERS
        block = pltpu.VMEM((planes, half, nx), jnp.float32)
        edge = pltpu.VMEM((exchanges, -(-planes // 8) * 8, nx), jnp.float32)
        dma = pltpu.SemaphoreType.DMA
        grad, adj, misfit = pl.pallas_call(
            functools.partial(kernel, n, rounds, float(n * own * ny * nx)),
            out_shape=(slab, slab, jax.ShapeDtypeStruct((8, 128), jnp.float32)),
            in_specs=[pl.BlockSpec(memory_space=pl.ANY)] * 4,
            out_specs=[pl.BlockSpec(memory_space=pltpu.VMEM)] * 3,
            scratch_shapes=[
                pltpu.VMEM((exchanges, planes, half + 2 * PAD, nx), jnp.float32),
                pltpu.VMEM((ITERS - 1, planes, half, nx), jnp.float32),
                pltpu.VMEM((2, exchanges, half, nx), jnp.float32),
                block, block, block, block, block,
                pltpu.VMEM((TILE, nx), jnp.float32),
                pltpu.VMEM((2 * rounds, 8, 128), jnp.float32),
                edge, edge,
                dma((4, 2)), dma((4, 2, CHUNKS)),
                dma((2, exchanges)), dma((2, exchanges, CHUNKS)),
                dma((exchanges,)), dma((exchanges,)),
                dma((2, 2)), dma((2, 2)),
                dma((rounds,)), dma((rounds,)),
            ],
            compiler_params=pltpu.CompilerParams(
                collective_id=0, has_side_effects=True, vmem_limit_bytes=67043328
            ),
        )(coefficient, initial_field, observed, misfit_weight)
        scale = misfit[0, 0]
        return grad / scale, adj / scale, scale

    placed = P("gz", None, None)
    return jax.shard_map(
        on_device,
        mesh=mesh,
        in_specs=(placed,) * 4,
        out_specs=(placed, placed, P()),
        check_vma=False,
    )
```

```python
import functools

import jax
import jax.numpy as jnp
from jax import lax
from jax.experimental import pallas as pl
from jax.experimental.pallas import tpu as pltpu
from jax.sharding import PartitionSpec as P

ITERS = 4
time_step = 0.125
MESH = pl.DeviceIdType.MESH
PAD = 8
TILE = 8
CHUNKS = 16


def kernel(n, rounds, cells, coef_hbm, init_hbm, obs_hbm, wgt_hbm, grad_out, adj_out, misfit_out,
           st, sl, halo, coef, obs, wgt, gacc, aacc, acc, part, edge_out, edge_in,
           in_send, in_recv, halo_send, halo_recv, edge_send, edge_recv,
           out_send, out_recv, psend_sem, precv_sem):
    own, ny, nx = coef_hbm.shape
    planes, half = 2 * own, ny // 2
    rows = half // CHUNKS
    exchanges = 2 * ITERS
    me = lax.axis_index("gz")
    q = me % 4
    base = me - q
    h, s = q // 2, q % 2
    lower, upper = me - 3 + 2 * s, me + 1 + 2 * s
    mate = me + 2 - 4 * h
    has_lo = lower >= 0
    has_hi = upper < n
    partners = []
    for r in range(rounds):
        bit = 1 << r
        partners.append(me + bit * (1 - 2 * ((me // bit) % 2)))

    barrier = pltpu.get_barrier_semaphore()

    def greet(device):
        pl.semaphore_signal(barrier, inc=1, device_id=(device,), device_id_type=MESH)

    for i in range(1, 4):
        greet(base + (q + i) % 4)
    for partner in partners[2:]:
        greet(partner)
    outside_lo = (s == 0) & has_lo
    outside_hi = (s == 1) & has_hi

    @pl.when(outside_lo)
    def _():
        greet(lower)

    @pl.when(outside_hi)
    def _():
        greet(upper)

    zero_rows = jnp.zeros((PAD, nx), jnp.float32)
    outer = pl.multiple_of(h * (PAD + half), PAD)
    inner = pl.multiple_of((1 - h) * (PAD + half), PAD)

    crossing = outside_lo | outside_hi

    @pl.when(crossing)
    def _():
        pl.semaphore_wait(barrier, rounds + 2)

    @pl.when(jnp.logical_not(crossing))
    def _():
        pl.semaphore_wait(barrier, rounds + 1)

    hbm = (init_hbm, coef_hbm, obs_hbm, wgt_hbm)
    held = (None, coef, obs, wgt)

    def place(side_half, j):
        return j if side_half == 1 else CHUNKS - 1 - j

    def feed(array, j):
        for to in range(2):
            dest = base + 2 * to + q // 2
            row = place(to, j) * rows
            slot = pl.ds(s * own, own)
            if array == 0:
                if isinstance(j, int) and j == 0:
                    start = row if to == 0 else half - PAD
                    src = init_hbm.at[:, pl.ds(start, rows + PAD), :]
                    dst = st.at[0, slot, pl.ds(PAD + row if to == 0 else 0, rows + PAD), :]
                else:
                    src = init_hbm.at[:, pl.ds(pl.multiple_of(to * half + row, PAD), rows), :]
                    dst = st.at[0, slot, pl.ds(pl.multiple_of(PAD + row, PAD), rows), :]
            else:
                src = hbm[array].at[:, pl.ds(pl.multiple_of(to * half + row, PAD), rows), :]
                dst = held[array].at[slot, pl.ds(pl.multiple_of(row, PAD), rows), :]
            arrived = in_recv.at[array, s, j]

            @pl.when(dest == me)
            def _():
                pltpu.make_async_copy(src, dst, arrived).start()

            @pl.when(dest != me)
            def _():
                pltpu.make_async_remote_copy(
                    src_ref=src, dst_ref=dst, send_sem=in_send.at[array, to], recv_sem=arrived,
                    device_id=(dest,), device_id_type=MESH,
                ).start()

    def await_copy(ref, sem):
        pltpu.make_async_copy(ref, ref, sem).wait()

    def fed(array, j, at):
        for slot in range(2):
            arrived = in_recv.at[array, slot, j]
            mine = pl.ds(slot * own, own)
            if array == 0:
                @pl.when(j == 0)
                def _():
                    start = pl.multiple_of((1 - h) * (PAD + at), PAD)
                    await_copy(st.at[0, mine, pl.ds(start, rows + PAD), :], arrived)

                @pl.when(j != 0)
                def _():
                    await_copy(st.at[0, mine, pl.ds(pl.multiple_of(PAD + at, PAD), rows), :], arrived)
            else:
                await_copy(held[array].at[mine, pl.ds(at, rows), :], arrived)

    for j in range(3):
        feed(0, j)
        feed(1, j)

    def clear_pad(e, carry):
        for p in range(planes):
            st[e, p, pl.ds(outer, PAD), :] = zero_rows
        return carry

    lax.fori_loop(0, exchanges, clear_pad, 0)

    def clear_halo(side):
        def clear(i, carry):
            e = i // (half // PAD)
            row = pl.multiple_of((i % (half // PAD)) * PAD, PAD)
            halo[side, e, pl.ds(row, PAD), :] = zero_rows
            return carry

        lax.fori_loop(0, exchanges * (half // PAD), clear, 0)

    @pl.when(jnp.logical_not(has_lo))
    def _():
        clear_halo(0)

    @pl.when(jnp.logical_not(has_hi))
    def _():
        clear_halo(1)

    acc[...] = jnp.zeros_like(acc)
    def send(e, at, j):
        here = pl.ds(at, rows)
        padded = pl.ds(pl.multiple_of(PAD + at, PAD), rows)

        def copy(side, device):
            pltpu.make_async_remote_copy(
                src_ref=st.at[e, (planes - 1) * (1 - side), padded, :],
                dst_ref=halo.at[side, e, here, :],
                send_sem=halo_send.at[side, e], recv_sem=halo_recv.at[side, e, j],
                device_id=(device,), device_id_type=MESH,
            ).start()

        @pl.when(has_hi)
        def _():
            copy(0, upper)

        @pl.when(has_lo)
        def _():
            copy(1, lower)

    def receive(e, at, j):
        here = pl.ds(at, rows)

        @pl.when(has_lo)
        def _():
            await_copy(halo.at[0, e, here, :], halo_recv.at[0, e, j])

        @pl.when(has_hi)
        def _():
            await_copy(halo.at[1, e, here, :], halo_recv.at[1, e, j])

    def edge_copy(e):
        return pltpu.make_async_remote_copy(
            src_ref=edge_out.at[e], dst_ref=edge_in.at[e],
            send_sem=edge_send.at[e], recv_sem=edge_recv.at[e],
            device_id=(mate,), device_id_type=MESH,
        )

    def stage_edge(e):
        at = pl.multiple_of(PAD + (1 - h) * (half - PAD), PAD)
        for p in range(planes):
            block = st[e, p, pl.ds(at, PAD), :]
            edge_out[e, p:p + 1, :] = jnp.where(h == 0, block[PAD - 1:PAD], block[0:1])

    def take_edge(e):
        edge_copy(e).wait_recv()
        for p in range(planes):
            st[e, p, pl.ds(inner, PAD), :] = jnp.broadcast_to(edge_in[e, p:p + 1, :], (PAD, nx))

    lane = lax.broadcasted_iota(jnp.int32, (TILE, nx), 1)
    leftmost = lane == 0
    rightmost = lane == nx - 1

    def laplace(e, p, row):
        here = pl.ds(row, TILE)
        padded = pl.ds(pl.multiple_of(row + PAD, PAD), TILE)
        tall = st[e, p, pl.ds(row, TILE + 2 * PAD), :]
        mid = tall[PAD:PAD + TILE]
        beside = tall[PAD + 1:PAD + 1 + TILE] + tall[PAD - 1:PAD - 1 + TILE]
        beside = beside + jnp.where(rightmost, 0.0, pltpu.roll(mid, nx - 1, 1))
        beside = beside + jnp.where(leftmost, 0.0, pltpu.roll(mid, 1, 1))
        above = st[e, p + 1, padded, :] if p + 1 < planes else halo[1, e, here, :]
        below = st[e, p - 1, padded, :] if p > 0 else halo[0, e, here, :]
        return mid, beside + above + below - 6.0 * mid

    def ship(which, source, target, m):
        at = pl.multiple_of((CHUNKS - 2 - 2 * m) * (1 - h) * rows + 2 * m * h * rows, PAD)
        for o in range(2):
            dest = base + 2 * s + o
            src = source.at[pl.ds(o * own, own), pl.ds(at, 2 * rows), :]
            dst = target.at[:, pl.ds(pl.multiple_of(h * half + at, PAD), 2 * rows), :]

            @pl.when(dest == me)
            def _():
                pltpu.make_async_copy(src, dst, out_recv.at[which, h]).start()

            @pl.when(dest != me)
            def _():
                pltpu.make_async_remote_copy(
                    src_ref=src, dst_ref=dst, send_sem=out_send.at[which, o],
                    recv_sem=out_recv.at[which, h], device_id=(dest,), device_id_type=MESH,
                ).start()

    def stage(e, j):
        at = pl.multiple_of((CHUNKS - 1 - j) * (1 - h) * rows + j * h * rows, PAD)
        if e == 0:
            fed(1, j, at)
        else:
            @pl.when(j == 0)
            def _():
                take_edge(e)
        if e == ITERS - 1:
            fed(2, j, at)
            fed(3, j, at)
        receive(e, at, j)

        def tile(t, carry):
            row = pl.multiple_of(at + t * TILE, TILE)
            here = pl.ds(row, TILE)
            padded = pl.ds(pl.multiple_of(row + PAD, PAD), TILE)
            for p in range(planes):
                mid, slope = laplace(e, p, row)
                if e < ITERS - 1:
                    sl[e, p, here, :] = slope
                    st[e + 1, p, padded, :] = mid + time_step * coef[p, here, :] * slope
                elif e == ITERS - 1:
                    c = coef[p, here, :]
                    resid = mid + time_step * c * slope - obs[p, here, :]
                    weighted = wgt[p, here, :] * resid
                    acc[...] += weighted * resid
                    aacc[p, here, :] = weighted
                    gacc[p, here, :] = time_step * weighted * slope
                    st[e + 1, p, padded, :] = c * weighted
                else:
                    lam = aacc[p, here, :] + time_step * slope
                    aacc[p, here, :] = lam
                    if e < exchanges - 1:
                        gacc[p, here, :] += time_step * lam * sl[exchanges - 2 - e, p, here, :]
                        st[e + 1, p, padded, :] = coef[p, here, :] * lam
            return carry

        lax.fori_loop(0, rows // TILE, tile, 0)
        if e < exchanges - 1:
            @pl.when(j == 0)
            def _():
                stage_edge(e + 1)

            send(e + 1, at, j)

            @pl.when(j == 0)
            def _():
                edge_copy(e + 1).start()

    def exchange(r):
        return pltpu.make_async_remote_copy(
            src_ref=part.at[2 * r], dst_ref=part.at[2 * r + 1],
            send_sem=psend_sem.at[r], recv_sem=precv_sem.at[r],
            device_id=(partners[r],), device_id_type=MESH,
        )

    def total_round(r):
        if r == 0:
            whole = acc[...]
            narrow = whole[:, 0:128]
            for i in range(1, nx // 128):
                narrow = narrow + whole[:, 128 * i:128 * i + 128]
            part[0] = narrow
        else:
            exchange(r - 1).wait_recv()
            part[2 * r] = part[2 * r - 2] + part[2 * r - 1]
        exchange(r).start()

    summed = CHUNKS + ITERS - 1
    ticks = CHUNKS + exchanges

    def tick(t, carry):
        @pl.when(t < CHUNKS)
        def _():
            at = pl.multiple_of((CHUNKS - 1 - t) * (1 - h) * rows + t * h * rows, PAD)
            fed(0, t, at)
            send(0, at, t)

        for e in range(exchanges):
            j = t - 1 - e

            @pl.when((j >= 0) & (j < CHUNKS))
            def _():
                stage(e, j)

        @pl.when(t + 3 < CHUNKS)
        def _():
            feed(0, t + 3)
            feed(1, t + 3)

        late = t + 2 - ITERS + 1

        @pl.when((late >= 0) & (late < CHUNKS))
        def _():
            feed(2, late)
            feed(3, late)

        for which, source, target, begin in ((0, gacc, grad_out, CHUNKS - 1), (1, aacc, adj_out, CHUNKS - 0)):
            m = t - begin

            @pl.when((m >= 0) & (m < CHUNKS // 2))
            def _():
                ship(which, source, target, m)

        for r in range(min(rounds, ticks - summed)):
            @pl.when(t == summed + r)
            def _():
                total_round(r)

        return carry

    lax.fori_loop(0, ticks, tick, 0)
    for r in range(ticks - summed, rounds):
        total_round(r)

    exchange(rounds - 1).wait_recv()
    whole = part[2 * rounds - 2] + part[2 * rounds - 1]
    whole = jnp.sum(jnp.sum(whole, axis=1, keepdims=True), axis=0, keepdims=True)
    misfit_out[...] = jnp.sqrt(jnp.broadcast_to(whole, (8, 128)) / cells + 1e-06)

    for which, target in enumerate((grad_out, adj_out)):
        for side in range(2):
            await_copy(target.at[:, pl.ds(side * half, half), :], out_recv.at[which, side])
    for which, source in enumerate((gacc, aacc)):
        for o in range(2):
            @pl.when(base + 2 * s + o != me)
            def _():
                await_copy(source.at[pl.ds(o * own, own)], out_send.at[which, o])
    for array in range(4):
        for to in range(2):
            @pl.when(base + 2 * to + q // 2 != me)
            def _():
                extra = PAD if array == 0 else 0
                await_copy(hbm[array].at[:, pl.ds(0, half + extra), :], in_send.at[array, to])
    for e in range(exchanges):
        @pl.when(has_hi)
        def _():
            await_copy(halo.at[0, e], halo_send.at[0, e])

        @pl.when(has_lo)
        def _():
            await_copy(halo.at[1, e], halo_send.at[1, e])
    for e in range(1, exchanges):
        edge_copy(e).wait_send()
    for r in range(rounds):
        exchange(r).wait_send()


def solution(mesh):
    n = mesh.shape["gz"]
    rounds = n.bit_length() - 1

    def on_device(coefficient, initial_field, observed, misfit_weight):
        own, ny, nx = coefficient.shape
        planes, half = 2 * own, ny // 2
        slab = jax.ShapeDtypeStruct(coefficient.shape, jnp.float32)
        exchanges = 2 * ITERS
        block = pltpu.VMEM((planes, half, nx), jnp.float32)
        edge = pltpu.VMEM((exchanges, planes, nx), jnp.float32)
        dma = pltpu.SemaphoreType.DMA
        grad, adj, misfit = pl.pallas_call(
            functools.partial(kernel, n, rounds, float(n * own * ny * nx)),
            out_shape=(slab, slab, jax.ShapeDtypeStruct((8, 128), jnp.float32)),
            in_specs=[pl.BlockSpec(memory_space=pl.ANY)] * 4,
            out_specs=[pl.BlockSpec(memory_space=pl.ANY)] * 2 + [pl.BlockSpec(memory_space=pltpu.VMEM)],
            scratch_shapes=[
                pltpu.VMEM((exchanges, planes, half + 2 * PAD, nx), jnp.float32),
                pltpu.VMEM((ITERS - 1, planes, half, nx), jnp.float32),
                pltpu.VMEM((2, exchanges, half, nx), jnp.float32),
                block, block, block, block, block,
                pltpu.VMEM((TILE, nx), jnp.float32),
                pltpu.VMEM((2 * rounds, 8, 128), jnp.float32),
                edge, edge,
                dma((4, 2)), dma((4, 2, CHUNKS)),
                dma((2, exchanges)), dma((2, exchanges, CHUNKS)),
                dma((exchanges,)), dma((exchanges,)),
                dma((2, 2)), dma((2, 2)),
                dma((rounds,)), dma((rounds,)),
            ],
            compiler_params=pltpu.CompilerParams(
                collective_id=0, has_side_effects=True, vmem_limit_bytes=48 * 1024 * 1024
            ),
        )(coefficient, initial_field, observed, misfit_weight)
        scale = misfit[0, 0]
        return grad / scale, adj / scale, scale

    placed = P("gz", None, None)
    return jax.shard_map(
        on_device,
        mesh=mesh,
        in_specs=(placed,) * 4,
        out_specs=(placed, placed, P()),
        check_vma=False,
    )
```

```python
import functools

import jax
import jax.numpy as jnp
from jax import lax
from jax.experimental import pallas as pl
from jax.experimental.pallas import tpu as pltpu
from jax.sharding import PartitionSpec as P

ITERS = 4
time_step = 0.125
MESH = pl.DeviceIdType.MESH
PAD = 8
TILE = 8
CHUNKS = 16


def kernel(n, rounds, cells, coef_hbm, init_hbm, obs_hbm, wgt_hbm, grad_out, adj_out, misfit_out,
           st, sl, halo, coef, obs, wgt, gacc, aacc, acc, part, edge_out, edge_in,
           in_send, in_recv, halo_send, halo_recv, edge_send, edge_recv,
           out_send, out_recv, psend_sem, precv_sem):
    own, ny, nx = coef_hbm.shape
    planes, half = 2 * own, ny // 2
    rows = half // CHUNKS
    exchanges = 2 * ITERS
    me = lax.axis_index("gz")
    q = me % 4
    base = me - q
    h, s = q // 2, q % 2
    lower, upper = me - 3 + 2 * s, me + 1 + 2 * s
    mate = me + 2 - 4 * h
    has_lo = lower >= 0
    has_hi = upper < n
    partners = []
    for r in range(rounds):
        bit = 1 << r
        partners.append(me + bit * (1 - 2 * ((me // bit) % 2)))

    barrier = pltpu.get_barrier_semaphore()

    def greet(device):
        pl.semaphore_signal(barrier, inc=1, device_id=(device,), device_id_type=MESH)

    for i in range(1, 4):
        greet(base + (q + i) % 4)
    for partner in partners[2:]:
        greet(partner)
    outside_lo = (s == 0) & has_lo
    outside_hi = (s == 1) & has_hi

    @pl.when(outside_lo)
    def _():
        greet(lower)

    @pl.when(outside_hi)
    def _():
        greet(upper)

    zero_rows = jnp.zeros((PAD, nx), jnp.float32)
    outer = pl.multiple_of(h * (PAD + half), PAD)
    inner = pl.multiple_of((1 - h) * (PAD + half), PAD)

    crossing = outside_lo | outside_hi

    @pl.when(crossing)
    def _():
        pl.semaphore_wait(barrier, rounds + 2)

    @pl.when(jnp.logical_not(crossing))
    def _():
        pl.semaphore_wait(barrier, rounds + 1)

    hbm = (init_hbm, coef_hbm, obs_hbm, wgt_hbm)
    held = (None, coef, obs, wgt)

    def place(side_half, j):
        return j if side_half == 1 else CHUNKS - 1 - j

    def feed(array, j):
        for to in range(2):
            dest = base + 2 * to + q // 2
            row = place(to, j) * rows
            slot = pl.ds(s * own, own)
            if array == 0:
                if isinstance(j, int) and j == 0:
                    start = row if to == 0 else half - PAD
                    src = init_hbm.at[:, pl.ds(start, rows + PAD), :]
                    dst = st.at[0, slot, pl.ds(PAD + row if to == 0 else 0, rows + PAD), :]
                else:
                    src = init_hbm.at[:, pl.ds(pl.multiple_of(to * half + row, PAD), rows), :]
                    dst = st.at[0, slot, pl.ds(pl.multiple_of(PAD + row, PAD), rows), :]
            else:
                src = hbm[array].at[:, pl.ds(pl.multiple_of(to * half + row, PAD), rows), :]
                dst = held[array].at[slot, pl.ds(pl.multiple_of(row, PAD), rows), :]
            arrived = in_recv.at[array, s, j]

            @pl.when(dest == me)
            def _():
                pltpu.make_async_copy(src, dst, arrived).start()

            @pl.when(dest != me)
            def _():
                pltpu.make_async_remote_copy(
                    src_ref=src, dst_ref=dst, send_sem=in_send.at[array, to], recv_sem=arrived,
                    device_id=(dest,), device_id_type=MESH,
                ).start()

    def await_copy(ref, sem):
        pltpu.make_async_copy(ref, ref, sem).wait()

    def fed(array, j, at):
        for slot in range(2):
            arrived = in_recv.at[array, slot, j]
            mine = pl.ds(slot * own, own)
            if array == 0:
                @pl.when(j == 0)
                def _():
                    start = pl.multiple_of((1 - h) * (PAD + at), PAD)
                    await_copy(st.at[0, mine, pl.ds(start, rows + PAD), :], arrived)

                @pl.when(j != 0)
                def _():
                    await_copy(st.at[0, mine, pl.ds(pl.multiple_of(PAD + at, PAD), rows), :], arrived)
            else:
                await_copy(held[array].at[mine, pl.ds(at, rows), :], arrived)

    for j in range(3):
        feed(0, j)
        feed(1, j)

    def clear_pad(e, carry):
        for p in range(planes):
            st[e, p, pl.ds(outer, PAD), :] = zero_rows
        return carry

    lax.fori_loop(0, exchanges, clear_pad, 0)

    def clear_halo(side):
        def clear(i, carry):
            e = i // (half // PAD)
            row = pl.multiple_of((i % (half // PAD)) * PAD, PAD)
            halo[side, e, pl.ds(row, PAD), :] = zero_rows
            return carry

        lax.fori_loop(0, exchanges * (half // PAD), clear, 0)

    @pl.when(jnp.logical_not(has_lo))
    def _():
        clear_halo(0)

    @pl.when(jnp.logical_not(has_hi))
    def _():
        clear_halo(1)

    acc[...] = jnp.zeros_like(acc)
    def send(e, at, j):
        here = pl.ds(at, rows)
        padded = pl.ds(pl.multiple_of(PAD + at, PAD), rows)

        def copy(side, device):
            pltpu.make_async_remote_copy(
                src_ref=st.at[e, (planes - 1) * (1 - side), padded, :],
                dst_ref=halo.at[side, e, here, :],
                send_sem=halo_send.at[side, e], recv_sem=halo_recv.at[side, e, j],
                device_id=(device,), device_id_type=MESH,
            ).start()

        @pl.when(has_hi)
        def _():
            copy(0, upper)

        @pl.when(has_lo)
        def _():
            copy(1, lower)

    def receive(e, at, j):
        here = pl.ds(at, rows)

        @pl.when(has_lo)
        def _():
            await_copy(halo.at[0, e, here, :], halo_recv.at[0, e, j])

        @pl.when(has_hi)
        def _():
            await_copy(halo.at[1, e, here, :], halo_recv.at[1, e, j])

    def edge_copy(e):
        return pltpu.make_async_remote_copy(
            src_ref=edge_out.at[e], dst_ref=edge_in.at[e],
            send_sem=edge_send.at[e], recv_sem=edge_recv.at[e],
            device_id=(mate,), device_id_type=MESH,
        )

    def stage_edge(e):
        at = pl.multiple_of(PAD + (1 - h) * (half - PAD), PAD)
        for p in range(planes):
            block = st[e, p, pl.ds(at, PAD), :]
            edge_out[e, p:p + 1, :] = jnp.where(h == 0, block[PAD - 1:PAD], block[0:1])

    def take_edge(e):
        edge_copy(e).wait_recv()
        for p in range(planes):
            st[e, p, pl.ds(inner, PAD), :] = jnp.broadcast_to(edge_in[e, p:p + 1, :], (PAD, nx))

    lane = lax.broadcasted_iota(jnp.int32, (TILE, nx), 1)
    leftmost = lane == 0
    rightmost = lane == nx - 1

    def laplace(e, p, row):
        here = pl.ds(row, TILE)
        padded = pl.ds(pl.multiple_of(row + PAD, PAD), TILE)
        tall = st[e, p, pl.ds(row, TILE + 2 * PAD), :]
        mid = tall[PAD:PAD + TILE]
        beside = tall[PAD + 1:PAD + 1 + TILE] + tall[PAD - 1:PAD - 1 + TILE]
        beside = beside + jnp.where(rightmost, 0.0, pltpu.roll(mid, nx - 1, 1))
        beside = beside + jnp.where(leftmost, 0.0, pltpu.roll(mid, 1, 1))
        above = st[e, p + 1, padded, :] if p + 1 < planes else halo[1, e, here, :]
        below = st[e, p - 1, padded, :] if p > 0 else halo[0, e, here, :]
        return mid, beside + above + below - 6.0 * mid

    def ship(which, source, target, m):
        at = pl.multiple_of((CHUNKS - 2 - 2 * m) * (1 - h) * rows + 2 * m * h * rows, PAD)
        for o in range(2):
            dest = base + 2 * s + o
            src = source.at[pl.ds(o * own, own), pl.ds(at, 2 * rows), :]
            dst = target.at[:, pl.ds(pl.multiple_of(h * half + at, PAD), 2 * rows), :]

            @pl.when(dest == me)
            def _():
                pltpu.make_async_copy(src, dst, out_recv.at[which, h]).start()

            @pl.when(dest != me)
            def _():
                pltpu.make_async_remote_copy(
                    src_ref=src, dst_ref=dst, send_sem=out_send.at[which, o],
                    recv_sem=out_recv.at[which, h], device_id=(dest,), device_id_type=MESH,
                ).start()

    def stage(e, j):
        at = pl.multiple_of((CHUNKS - 1 - j) * (1 - h) * rows + j * h * rows, PAD)
        if e == 0:
            fed(1, j, at)
        else:
            @pl.when(j == 0)
            def _():
                take_edge(e)
        if e == ITERS - 1:
            fed(2, j, at)
            fed(3, j, at)
        receive(e, at, j)

        def tile(t, carry):
            row = pl.multiple_of(at + t * TILE, TILE)
            here = pl.ds(row, TILE)
            padded = pl.ds(pl.multiple_of(row + PAD, PAD), TILE)
            for p in range(planes):
                mid, slope = laplace(e, p, row)
                if e < ITERS - 1:
                    sl[e, p, here, :] = slope
                    st[e + 1, p, padded, :] = mid + time_step * coef[p, here, :] * slope
                elif e == ITERS - 1:
                    c = coef[p, here, :]
                    resid = mid + time_step * c * slope - obs[p, here, :]
                    weighted = wgt[p, here, :] * resid
                    acc[...] += weighted * resid
                    aacc[p, here, :] = weighted
                    gacc[p, here, :] = time_step * weighted * slope
                    st[e + 1, p, padded, :] = c * weighted
                else:
                    lam = aacc[p, here, :] + time_step * slope
                    aacc[p, here, :] = lam
                    if e < exchanges - 1:
                        gacc[p, here, :] += time_step * lam * sl[exchanges - 2 - e, p, here, :]
                        st[e + 1, p, padded, :] = coef[p, here, :] * lam
            return carry

        lax.fori_loop(0, rows // TILE, tile, 0)
        if e < exchanges - 1:
            @pl.when(j == 0)
            def _():
                stage_edge(e + 1)

            send(e + 1, at, j)

            @pl.when(j == 0)
            def _():
                edge_copy(e + 1).start()

    def exchange(r):
        return pltpu.make_async_remote_copy(
            src_ref=part.at[2 * r], dst_ref=part.at[2 * r + 1],
            send_sem=psend_sem.at[r], recv_sem=precv_sem.at[r],
            device_id=(partners[r],), device_id_type=MESH,
        )

    def total_round(r):
        if r == 0:
            whole = acc[...]
            narrow = whole[:, 0:128]
            for i in range(1, nx // 128):
                narrow = narrow + whole[:, 128 * i:128 * i + 128]
            part[0] = narrow
        else:
            exchange(r - 1).wait_recv()
            part[2 * r] = part[2 * r - 2] + part[2 * r - 1]
        exchange(r).start()

    summed = CHUNKS + ITERS - 1
    ticks = CHUNKS + exchanges

    def tick(t, carry):
        @pl.when(t < CHUNKS)
        def _():
            at = pl.multiple_of((CHUNKS - 1 - t) * (1 - h) * rows + t * h * rows, PAD)
            fed(0, t, at)
            send(0, at, t)

        for e in range(exchanges):
            j = t - 1 - e

            @pl.when((j >= 0) & (j < CHUNKS))
            def _():
                stage(e, j)

        @pl.when(t + 3 < CHUNKS)
        def _():
            feed(0, t + 3)
            feed(1, t + 3)

        late = t + 2 - ITERS + 1

        @pl.when((late >= 0) & (late < CHUNKS))
        def _():
            feed(2, late)
            feed(3, late)

        for which, source, target, begin in ((0, gacc, grad_out, CHUNKS - 2), (1, aacc, adj_out, CHUNKS - 1)):
            m, final = t - begin, CHUNKS // 2 - 1

            @pl.when((m >= 0) & (m < final))
            def _():
                ship(which, source, target, m)

            @pl.when(m == final + 1)
            def _():
                ship(which, source, target, final)

        for r in range(min(rounds, ticks - summed)):
            @pl.when(t == summed + r)
            def _():
                total_round(r)

        return carry

    lax.fori_loop(0, ticks, tick, 0)
    for r in range(ticks - summed, rounds):
        total_round(r)

    exchange(rounds - 1).wait_recv()
    whole = part[2 * rounds - 2] + part[2 * rounds - 1]
    whole = jnp.sum(jnp.sum(whole, axis=1, keepdims=True), axis=0, keepdims=True)
    misfit_out[...] = jnp.sqrt(jnp.broadcast_to(whole, (8, 128)) / cells + 1e-06)

    for which, target in enumerate((grad_out, adj_out)):
        for side in range(2):
            await_copy(target.at[:, pl.ds(side * half, half), :], out_recv.at[which, side])
    for which, source in enumerate((gacc, aacc)):
        for o in range(2):
            @pl.when(base + 2 * s + o != me)
            def _():
                await_copy(source.at[pl.ds(o * own, own)], out_send.at[which, o])
    for array in range(4):
        for to in range(2):
            @pl.when(base + 2 * to + q // 2 != me)
            def _():
                extra = PAD if array == 0 else 0
                await_copy(hbm[array].at[:, pl.ds(0, half + extra), :], in_send.at[array, to])
    for e in range(exchanges):
        @pl.when(has_hi)
        def _():
            await_copy(halo.at[0, e], halo_send.at[0, e])

        @pl.when(has_lo)
        def _():
            await_copy(halo.at[1, e], halo_send.at[1, e])
    for e in range(1, exchanges):
        edge_copy(e).wait_send()
    for r in range(rounds):
        exchange(r).wait_send()


def solution(mesh):
    n = mesh.shape["gz"]
    rounds = n.bit_length() - 1

    def on_device(coefficient, initial_field, observed, misfit_weight):
        own, ny, nx = coefficient.shape
        planes, half = 2 * own, ny // 2
        slab = jax.ShapeDtypeStruct(coefficient.shape, jnp.float32)
        exchanges = 2 * ITERS
        block = pltpu.VMEM((planes, half, nx), jnp.float32)
        edge = pltpu.VMEM((exchanges, planes, nx), jnp.float32)
        dma = pltpu.SemaphoreType.DMA
        grad, adj, misfit = pl.pallas_call(
            functools.partial(kernel, n, rounds, float(n * own * ny * nx)),
            out_shape=(slab, slab, jax.ShapeDtypeStruct((8, 128), jnp.float32)),
            in_specs=[pl.BlockSpec(memory_space=pl.ANY)] * 4,
            out_specs=[pl.BlockSpec(memory_space=pl.ANY)] * 2 + [pl.BlockSpec(memory_space=pltpu.VMEM)],
            scratch_shapes=[
                pltpu.VMEM((exchanges, planes, half + 2 * PAD, nx), jnp.float32),
                pltpu.VMEM((ITERS - 1, planes, half, nx), jnp.float32),
                pltpu.VMEM((2, exchanges, half, nx), jnp.float32),
                block, block, block, block, block,
                pltpu.VMEM((TILE, nx), jnp.float32),
                pltpu.VMEM((2 * rounds, 8, 128), jnp.float32),
                edge, edge,
                dma((4, 2)), dma((4, 2, CHUNKS)),
                dma((2, exchanges)), dma((2, exchanges, CHUNKS)),
                dma((exchanges,)), dma((exchanges,)),
                dma((2, 2)), dma((2, 2)),
                dma((rounds,)), dma((rounds,)),
            ],
            compiler_params=pltpu.CompilerParams(
                collective_id=0, has_side_effects=True, vmem_limit_bytes=48 * 1024 * 1024
            ),
        )(coefficient, initial_field, observed, misfit_weight)
        scale = misfit[0, 0]
        return grad / scale, adj / scale, scale

    placed = P("gz", None, None)
    return jax.shard_map(
        on_device,
        mesh=mesh,
        in_specs=(placed,) * 4,
        out_specs=(placed, placed, P()),
        check_vma=False,
    )
```
